32 devices in a mesh: expert: 8 (over z, y), replica: 2 (over core), group: 2 (over x).
Axes of the slice: x: 2, y: 2, z: 4, core: 2. Of those that a mesh axis runs over, the one named last changes fastest.
Arguments:
- tokens: bfloat16 [1536, 4096], P('expert', 'group'), may hold values from -6 to 6
- expert_ids: int32 [1536, 8], P('expert'), may hold values from 0 to 127, all different within a row; in each aligned block of 192 rows (0 to 191, 192 to 383, ...) at most 15 rows name the same one
- route_gates: float32 [1536, 8], P('expert'), may hold values from 0.03 to 0.5
- member_order: int32 [8], replicated, may hold values from 0 to 7, each once
- teach_gate: bfloat16 [8, 1536, 4096], P('expert', 'replica', 'group'), may hold values from -0.09375 to 0.09375
- teach_up: bfloat16 [8, 1536, 4096], P('expert', 'replica', 'group'), may hold values from -0.09375 to 0.09375
- teach_down: bfloat16 [8, 1536, 4096], P('expert', 'replica', 'group'), may hold values from -0.15625 to 0.15625
- stud_gate: bfloat16 [8, 1536, 2048], P('expert', 'replica', 'group'), may hold values from -0.09375 to 0.09375
- stud_up: bfloat16 [8, 1536, 2048], P('expert', 'replica', 'group'), may hold values from -0.09375 to 0.09375
- stud_down: bfloat16 [8, 1536, 2048], P('expert', 'replica', 'group'), may hold values from -0.15625 to 0.15625
Outputs:
- residual: float32 [1536, 4096], P('expert', ('group', 'replica'))
- grad_gate: bfloat16 [8, 1536, 2048], P('expert', 'replica', 'group')
- grad_up: bfloat16 [8, 1536, 2048], P('expert', 'replica', 'group')
- grad_down: bfloat16 [8, 1536, 2048], P('expert', 'replica', 'group')
The draws below stay inside these ranges and needn't reach their ends.
Inputs may be any that keep to these rules, and one draw needn't show every extreme that they name: `expert_ids`: each row names 8 different experts. Within each aligned block of 192 rows no expert is named by more than 15 rows. Only experts below 8 are in the window. `member_order`: every teacher expert of the window appears once.
All inputs are finite; a program needn't handle non-finite values.
Results may differ from the reference program's by a relative error of at most 0.025.
Values may be sent and summed in bfloat16 or wider, within the bound.
No kernel may reach another device: no remote copies, remote signals or barrier semaphores. Data moves between devices by JAX's collectives and lax.ppermute only.
A program may use at most 128 MiB of HBM per device.

```python
import math
import jax
import jax.numpy as jnp
import numpy as np
from jax import lax

D = 4096
FF = 1536
EXPERTS = 128
TOPK = 8
TOK_DEV = 192
CAP = 15
TOKENS = 1536
TEACH = 8
STUD = 4
SUB = 512
N_EXPERT = 8
N_REPLICA = 2


def steps_of(own_key, dims, cuts, least, high):
    loudness, own = 1.0, jax.random.fold_in(own_key, 6)
    for dim, parts in cuts:
        steps = jnp.exp(jax.random.uniform(jax.random.fold_in(own, dim), (parts,), jnp.float32, least / len(cuts), high / len(cuts)))
        loudness = loudness * jnp.repeat(steps, dims[dim] // parts).reshape([-1 if axis == dim else 1 for axis in range(len(dims))])
    return loudness


def assign_block(rng, own, number, rows, count, top, limit, lean):
    sequence = jax.random.permutation(rng, count)
    packed, common = load_shares(count, rows * top, limit, lean, True), load_shares(count, rows * top, limit, lean, False)
    places = jnp.arange(count)

    def named(lengths, rotation):
        used = int((lengths > 0).sum())
        fixed = max(1, used // 4)
        moved = fixed + (places - fixed + rotation * (used - fixed)) % max(1, count - fixed)
        return jnp.zeros((count,), jnp.int32).at[sequence[jnp.where(places < fixed, places, moved)]].set(jnp.asarray(lengths, jnp.int32))

    lengths = jnp.where(number % 4 == 0, named(packed, number // 4), named(common, number - number // 4 - 1))
    mixed = jax.random.permutation(jax.random.fold_in(own, 3), count)
    source_of, taker = mixed[0:count // 2 * 2:2], mixed[1:count // 2 * 2:2]
    room = jnp.minimum(lengths[source_of] - 1, limit - lengths[taker]) // 2
    room = jnp.where((source_of == sequence[0]) | (taker == sequence[0]) | (lengths[taker] == 0), 0, jnp.maximum(room, 0))
    moved = jax.random.randint(jax.random.fold_in(own, 4), (count // 2,), 0, 1 << 20) % (room + 1)
    lengths = lengths.at[source_of].add(-moved).at[taker].add(moved)
    members = jnp.searchsorted(jnp.cumsum(lengths), jnp.arange(rows * top), side="right").astype(jnp.int32)
    grid = members.reshape(top, rows).T
    grid = grid[jax.random.permutation(jax.random.fold_in(own, 1), rows)]
    rotation = jax.random.randint(jax.random.fold_in(own, 2), (rows, 1), 0, top)
    return jnp.take_along_axis(grid, (jnp.arange(top)[None, :] + rotation) % top, axis=1)


def load_shares(amount, total, bound, skew, full):
    loads = [(1 << 20) // math.isqrt(grade ** skew) + 1 for grade in range(1, amount + 1)]
    largest = bound if full else min(bound, max(-(-total // amount), total * loads[0] // sum(loads)))
    least = 1 if total - largest >= amount - 1 else 0
    given, surplus = [largest] + [least] * (amount - 1), total - largest - least * (amount - 1)
    while surplus > 0:
        movable = [i for i in range(1, amount) if given[i] < largest] or [i for i in range(1, amount) if given[i] < bound]
        whole, remaining = sum([loads[i] for i in movable]), surplus
        for i in movable:
            addition = min(bound - given[i], max(1, remaining * loads[i] // whole), surplus)
            given[i] = given[i] + addition
            surplus = surplus - addition
    return np.array(given)


def normal_values(key, shape, scale, bound, shards=(), held_as=jnp.bfloat16):
    drawn = jax.random.normal(key, shape, jnp.float32) * scale
    if len(shards) > 0:
        drawn = steps_of(key, shape, shards, -0.22, 0.18) * drawn
    return jnp.clip(drawn, min=-bound, max=bound).astype(held_as)


def setup_inputs(seed: int = 0) -> dict:
    arg_keys = jax.random.split(jax.random.key(seed), 11)
    tokens = normal_values(arg_keys[0], (TOKENS, D), 1.0, 6.0, ((0, 8), (1, 2)))
    expert_ids_keys = jax.random.split(jax.random.fold_in(arg_keys[1], 1), TOKENS // TOK_DEV)
    expert_ids_turns = jax.random.permutation(jax.random.fold_in(arg_keys[1], 3), TOKENS // TOK_DEV)
    expert_ids = jax.vmap(lambda own, number: assign_block(jax.random.fold_in(arg_keys[1], 2), own, number, TOK_DEV, EXPERTS, TOPK, CAP, 2))(expert_ids_keys, expert_ids_turns).reshape((TOKENS, TOPK))
    route_gates = jnp.clip(jnp.exp(math.log(0.5) - 2.8134107 * jax.random.uniform(arg_keys[2], (TOKENS, TOPK), jnp.float32) ** steps_of(arg_keys[2], (TOKENS, TOPK), ((0, 8),), -0.2, 0.2)), 0.03, 0.5)
    member_order = jax.random.permutation(arg_keys[3], TEACH).astype(jnp.int32)
    teach_gate = normal_values(arg_keys[4], (TEACH, FF, D), D ** -0.5, 0.09375, ((0, 8), (1, 2), (2, 2)))
    teach_up = normal_values(arg_keys[5], (TEACH, FF, D), D ** -0.5, 0.09375, ((0, 8), (1, 2), (2, 2)))
    teach_down = normal_values(arg_keys[6], (TEACH, FF, D), FF ** -0.5, 0.15625, ((0, 8), (1, 2), (2, 2)))
    stud_gate = normal_values(arg_keys[7], (2 * STUD, FF, D // 2), D ** -0.5, 0.09375, ((0, 8), (1, 2), (2, 2)))
    stud_up = normal_values(arg_keys[8], (2 * STUD, FF, D // 2), D ** -0.5, 0.09375, ((0, 8), (1, 2), (2, 2)))
    stud_down = normal_values(arg_keys[9], (2 * STUD, FF, D // 2), FF ** -0.5, 0.15625, ((0, 8), (1, 2), (2, 2)))
    return {"tokens": tokens, "expert_ids": expert_ids, "route_gates": route_gates, "member_order": member_order, "teach_gate": teach_gate, "teach_up": teach_up, "teach_down": teach_down, "stud_gate": stud_gate, "stud_up": stud_up, "stud_down": stud_down}


def expert_slots(flat_ids, expert, slot_limit):
    pair_count = flat_ids.shape[0]
    chosen = flat_ids == expert
    rank_rows = jnp.cumsum(chosen.astype(jnp.int32)) - 1
    target = jnp.where(chosen, rank_rows, slot_limit).astype(jnp.int32)
    slot_table = jnp.full((slot_limit,), pair_count, jnp.int32)
    return slot_table.at[target].set(jnp.arange(pair_count, dtype=jnp.int32), mode="drop")


def full_rows(pair_block):
    shaped = pair_block.reshape(2, 2, N_REPLICA, SUB, FF)
    return shaped.transpose(1, 2, 0, 3, 4).reshape(D, FF)


def pack_rows(matrix):
    shaped = matrix.reshape(2, N_REPLICA, 2, SUB, FF)
    return shaped.transpose(2, 0, 1, 3, 4).reshape(2, D // 2, FF)


def full_cols(pair_block):
    shaped = pair_block.reshape(2, FF, 2, N_REPLICA, SUB)
    return shaped.transpose(1, 2, 3, 0, 4).reshape(FF, D)


def pack_cols(matrix):
    shaped = matrix.reshape(FF, 2, N_REPLICA, 2, SUB)
    return shaped.transpose(3, 0, 1, 2, 4).reshape(2, FF, D // 2)


def expert_forward(picked, gate_w, up_w, down_w):
    gate_pre = jnp.dot(picked, gate_w, preferred_element_type=jnp.float32)
    up_pre = jnp.dot(picked, up_w, preferred_element_type=jnp.float32)
    hidden = (gate_pre * jax.nn.sigmoid(gate_pre) * up_pre).astype(jnp.bfloat16)
    pieces = hidden.reshape(hidden.shape[0], N_REPLICA, FF // N_REPLICA).astype(jnp.float32)
    blocks = down_w.reshape(N_REPLICA, FF // N_REPLICA, D).astype(jnp.float32)
    partials = jnp.einsum("lrf,rfd->lrd", pieces, blocks).astype(jnp.bfloat16)
    partials = lax.optimization_barrier(partials)
    return jnp.sum(partials.astype(jnp.float32), axis=1)


def reference(tokens, expert_ids, route_gates, member_order, teach_gate, teach_up, teach_down, stud_gate, stud_up, stud_down):
    slot_limit = N_EXPERT * CAP
    flat_ids = expert_ids.reshape(-1)
    flat_gates = route_gates.reshape(-1)
    pair_count = flat_ids.shape[0]

    def gather_rows(merged):
        member_one = member_order[2 * merged]
        member_two = member_order[2 * merged + 1]
        slot_table = jnp.concatenate([expert_slots(flat_ids, member_one, slot_limit), expert_slots(flat_ids, member_two, slot_limit)])
        filled = slot_table < pair_count
        clamped = jnp.minimum(slot_table, pair_count - 1).astype(jnp.int32)
        token_index = (clamped // TOPK).astype(jnp.int32)
        weights = jnp.where(filled, flat_gates[clamped], jnp.zeros((), jnp.float32))
        picked = jnp.where(filled[:, None], tokens[token_index], jnp.zeros((), jnp.bfloat16))
        return member_one, member_two, token_index, weights, picked

    def merged_weights(merged):
        gate_w = full_rows(lax.dynamic_slice_in_dim(stud_gate, 2 * merged, 2, 0).transpose(0, 2, 1))
        up_w = full_rows(lax.dynamic_slice_in_dim(stud_up, 2 * merged, 2, 0).transpose(0, 2, 1))
        down_w = full_cols(lax.dynamic_slice_in_dim(stud_down, 2 * merged, 2, 0))
        return gate_w, up_w, down_w

    def forward_step(residual, merged):
        member_one, member_two, token_index, weights, picked = gather_rows(merged)
        teach_one = expert_forward(picked[:slot_limit], teach_gate[member_one].T, teach_up[member_one].T, teach_down[member_one])
        teach_two = expert_forward(picked[slot_limit:], teach_gate[member_two].T, teach_up[member_two].T, teach_down[member_two])
        teach_out = jnp.concatenate([teach_one, teach_two], axis=0)
        gate_w, up_w, down_w = merged_weights(merged)
        stud_out = expert_forward(picked, gate_w, up_w, down_w)
        term_rows = weights[:, None] * (stud_out - teach_out)
        return residual.at[token_index].add(term_rows), None

    residual, _ = lax.scan(forward_step, jnp.zeros((TOKENS, D), jnp.float32), jnp.arange(STUD, dtype=jnp.int32))

    def backward_step(merged):
        member_one, member_two, token_index, weights, picked = gather_rows(merged)
        gate_w, up_w, down_w = merged_weights(merged)
        gate_pre = jnp.dot(picked, gate_w, preferred_element_type=jnp.float32)
        up_pre = jnp.dot(picked, up_w, preferred_element_type=jnp.float32)
        sigmoid_gate = jax.nn.sigmoid(gate_pre)
        hidden = (gate_pre * sigmoid_gate * up_pre).astype(jnp.bfloat16)
        out_grad = (weights[:, None] * residual[token_index]).astype(jnp.bfloat16)
        back_hidden = lax.dot_general(out_grad, down_w, (((1,), (1,)), ((), ())), preferred_element_type=jnp.float32)
        gate_rows = (back_hidden * up_pre * sigmoid_gate * (1.0 + gate_pre * (1.0 - sigmoid_gate))).astype(jnp.bfloat16)
        up_rows = (back_hidden * gate_pre * sigmoid_gate).astype(jnp.bfloat16)
        inner = (((0,), (0,)), ((), ()))
        grad_gate = lax.dot_general(picked, gate_rows, inner, preferred_element_type=jnp.float32)
        grad_up = lax.dot_general(picked, up_rows, inner, preferred_element_type=jnp.float32)
        grad_down = lax.dot_general(hidden, out_grad, inner, preferred_element_type=jnp.float32)
        return (pack_rows(grad_gate).transpose(0, 2, 1).astype(jnp.bfloat16), pack_rows(grad_up).transpose(0, 2, 1).astype(jnp.bfloat16), pack_cols(grad_down).astype(jnp.bfloat16))

    gradients = lax.map(backward_step, jnp.arange(STUD, dtype=jnp.int32))
    grad_gate = gradients[0].reshape(2 * STUD, FF, D // 2)
    grad_up = gradients[1].reshape(2 * STUD, FF, D // 2)
    grad_down = gradients[2].reshape(2 * STUD, FF, D // 2)
    return (residual, grad_gate, grad_up, grad_down)
```

```python
import jax
import jax.numpy as jnp
from jax import lax
from jax.experimental import pallas as pl
from jax.experimental.pallas import tpu as pltpu
from jax.sharding import PartitionSpec as P

SLOT = 16


BF16 = jnp.bfloat16
F32 = jnp.float32


def swap(block, axis):
    count = lax.axis_size(axis)
    return lax.ppermute(block, axis, [(place, place ^ 1) for place in range(count)])


def exchange(block):
    return lax.all_to_all(block, "expert", split_axis=0, concat_axis=0, tiled=True)


def contract(left, right, dims):
    return lax.dot_general(left, right, ((dims[:1], dims[1:]), ((), ())), preferred_element_type=F32)


def call(body, outs, ins, scratch=(), smem=0, flops=0):
    specs = [pl.BlockSpec(memory_space=pltpu.SMEM)] * smem
    specs += [pl.BlockSpec(memory_space=pltpu.VMEM)] * (len(ins) - smem)
    moved = sum(x.size * x.dtype.itemsize for x in (*ins, *outs))
    return pl.pallas_call(
        body,
        out_shape=outs,
        in_specs=specs,
        out_specs=[pl.BlockSpec(memory_space=pltpu.VMEM)] * len(outs),
        scratch_shapes=scratch,
        name=body.__name__,
        cost_estimate=pl.CostEstimate(flops=flops, bytes_accessed=moved, transcendentals=0),
    )(*ins)


def struct(dtype, *shape):
    return jax.ShapeDtypeStruct(shape, dtype)


def spread_members(order, source, target, to_slots):
    owners, _, narrow = target.shape if not to_slots else source.shape
    for dest in range(owners):
        columns = slice(dest % 2 * narrow, (dest % 2 + 1) * narrow)
        for member in range(2):
            start = pl.multiple_of(order[dest // 2 * 2 + member] * SLOT, SLOT)
            rows = slice(member * SLOT, (member + 1) * SLOT)
            if to_slots:
                target[pl.ds(start, SLOT), columns] = source[dest, rows, :]
            else:
                target[dest, rows, :] = source[pl.ds(start, SLOT), columns]


def route(order, ids, gates, tokens, send, select, weight, picked):
    count, top = ids.shape
    owners, _, narrow = send.shape
    slots = select.shape[1]
    place = lax.broadcasted_iota(jnp.int32, (count, slots), 1)
    expert = place // SLOT
    slot = (place % SLOT).astype(F32)
    member = jnp.zeros((count, slots), F32)
    gate = jnp.zeros((count, slots), F32)
    for choice in range(top):
        hit = ids[:, choice : choice + 1] == expert
        member = jnp.where(hit, 1.0, member)
        gate = jnp.where(hit, gates[:, choice : choice + 1], gate)
    before = lax.broadcasted_iota(jnp.int32, (count, count), 0) > lax.broadcasted_iota(
        jnp.int32, (count, count), 1
    )
    rank = contract(before.astype(F32).astype(BF16), member.astype(BF16), (1, 0))
    chosen = (member > 0.0) & (rank == slot)
    onehot = jnp.where(chosen, 1.0, 0.0).astype(BF16)
    select[...] = onehot
    weight[...] = jnp.sum(jnp.where(chosen, gate, 0.0), axis=0, keepdims=True)
    start = pl.multiple_of(lax.axis_index("replica") * 2 * narrow, 2 * narrow)
    picked[...] = contract(onehot, tokens[:, pl.ds(start, 2 * narrow)], (0, 0)).astype(BF16)
    spread_members(order, picked, send, False)
    for dest in range(owners):
        rows = slice(dest * SLOT, (dest + 1) * SLOT)
        send[dest, 2 * SLOT : 3 * SLOT, :] = picked[rows, :narrow]
        send[dest, 3 * SLOT :, :] = picked[rows, narrow:]


def student_in(own, other, gate, up, first, second, rows):
    owners, _, narrow = own.shape
    half = owners * SLOT
    replica = lax.axis_index("replica")
    for part, at in ((own, replica), (other, 1 - replica)):
        columns = pl.ds(pl.multiple_of(at * narrow, narrow), narrow)
        rows[:, columns] = part[:, : 2 * SLOT, :].reshape(2 * half, narrow)
    for index, matrix in enumerate((gate, up)):
        pre = contract(rows[...], matrix[0], (1, 1)).astype(BF16)
        first[index] = pre[:half]
        second[index] = pre[half:]


def teacher_in(own, other, gate, up, pre, rows):
    owners, _, narrow = own.shape
    replica = lax.axis_index("replica")
    for part, at in ((own, replica), (other, 1 - replica)):
        for piece in range(2):
            start = pl.multiple_of((2 * at + piece) * narrow, narrow)
            block = part[:, (2 + piece) * SLOT : (3 + piece) * SLOT, :]
            rows[:, pl.ds(start, narrow)] = block.reshape(owners * SLOT, narrow)
    for index, matrix in enumerate((gate, up)):
        pre[index] = contract(rows[...], matrix[0], (1, 1)).astype(BF16)


def hidden_of(gate, up):
    return (gate * jax.nn.sigmoid(gate) * up).astype(BF16)


def divide(hidden, down, keep, send):
    width = keep.shape[1]
    replica = lax.axis_index("replica")
    mine = pl.ds(pl.multiple_of(replica * width, width), width)
    theirs = pl.ds(pl.multiple_of((1 - replica) * width, width), width)
    send[...] = contract(hidden, down[0, :, theirs], (1, 0)).astype(BF16)
    keep[...] = contract(hidden, down[0, :, mine], (1, 0))


def student_out(first, first_got, second, second_got, down, keep, send, hidden):
    half = first.shape[1]
    for at, (own, got) in enumerate(((first, first_got), (second, second_got))):
        gate, up = (own[i].astype(F32) + got[i].astype(F32) for i in range(2))
        hidden[at * half : (at + 1) * half, :] = hidden_of(gate, up)
    divide(hidden[...], down, keep, send)


def teacher_out(own, got, down, keep, send):
    gate, up = (own[i].astype(F32) + got[i].astype(F32) for i in range(2))
    divide(hidden_of(gate, up), down, keep, send)


def join(stud, stud_got, teach, teach_got, send):
    owners, _, narrow = send.shape
    total = (stud[...] + stud_got[...].astype(F32)).astype(BF16)
    send[:, : 2 * SLOT, :] = total.reshape(owners, 2 * SLOT, narrow)
    total = (teach[...] + teach_got[...].astype(F32)).astype(BF16)
    for piece in range(2):
        block = total[:, piece * narrow : (piece + 1) * narrow].reshape(owners, SLOT, narrow)
        send[:, (2 + piece) * SLOT : (3 + piece) * SLOT, :] = block


def halves(value):
    high = value.astype(BF16)
    return high, (value - high.astype(F32)).astype(BF16)


def combine(order, back, select, weight, residual, send, stud, teach):
    owners, _, narrow = back.shape
    slots = select.shape[1]
    spread_members(order, back, stud, True)
    for dest in range(owners):
        rows = slice(dest * SLOT, (dest + 1) * SLOT)
        teach[rows, :narrow] = back[dest, 2 * SLOT : 3 * SLOT, :]
        teach[rows, narrow:] = back[dest, 3 * SLOT :, :]
    scale = jnp.broadcast_to(weight[...], (128, slots)).T[:, :1]
    high, low = halves(scale * (stud[...].astype(F32) - teach[...].astype(F32)))
    onehot = select[...]
    total = contract(onehot, high, (1, 0)) + contract(onehot, low, (1, 0))
    residual[...] = total
    high, low = halves(total)
    rows = contract(onehot, high, (0, 0)) + contract(onehot, low, (0, 0))
    stud[...] = (scale * rows).astype(BF16)
    spread_members(order, stud, send, False)


def hidden_back(own, other, down, first, second, rows):
    owners, _, narrow = own.shape
    half = owners * SLOT
    replica = lax.axis_index("replica")
    for part, at in ((own, replica), (other, 1 - replica)):
        columns = pl.ds(pl.multiple_of(at * narrow, narrow), narrow)
        rows[:, columns] = part[...].reshape(2 * half, narrow)
    back = contract(rows[...], down[0], (1, 1)).astype(BF16)
    first[...] = back[:half]
    second[...] = back[half:]


def down_grad(hidden, rows, out):
    out[0] = contract(hidden[...], rows[...], (0, 0)).astype(BF16)


def grads(first, first_got, second, second_got, a_own, a_got, b_own, b_got, rows, gate_out, up_out, left):
    half = a_own.shape[0]
    pairs = ((first, first_got, a_own, a_got), (second, second_got, b_own, b_got))
    for at, (pre, pre_got, own, got) in enumerate(pairs):
        gate, up = (pre[i].astype(F32) + pre_got[i].astype(F32) for i in range(2))
        back = own[...].astype(F32) + got[...].astype(F32)
        sig = jax.nn.sigmoid(gate)
        block = slice(at * half, (at + 1) * half)
        left[0, block, :] = (back * up * sig * (1.0 + gate * (1.0 - sig))).astype(BF16)
        left[1, block, :] = (back * gate * sig).astype(BF16)
    gate_out[0] = contract(left[0], rows[...], (0, 0)).astype(BF16)
    up_out[0] = contract(left[1], rows[...], (0, 0)).astype(BF16)


def sum_bf16(own, got):
    return (own.astype(F32) + got.astype(F32)).astype(BF16)


def shards(tokens, expert_ids, route_gates, member_order, teach_gate, teach_up, teach_down, stud_gate, stud_up, stud_down):
    owners = lax.axis_size("expert")
    count, half_width = tokens.shape
    _, units, width = stud_gate.shape
    block = half_width // 2
    narrow = width // 2
    slots = owners * SLOT
    full = 2 * slots
    send, select, weight = call(
        route,
        [struct(BF16, owners, 4 * SLOT, narrow), struct(BF16, count, slots), struct(F32, 1, slots)],
        [member_order, expert_ids, route_gates, tokens],
        [pltpu.VMEM((slots, block), BF16)],
        smem=1,
        flops=2 * slots * count * block,
    )
    own = exchange(send)
    other = swap(own, "replica")
    first, second, stud_rows = call(
        student_in,
        [struct(BF16, 2, slots, units), struct(BF16, 2, slots, units), struct(BF16, full, width)],
        [own, other, stud_gate, stud_up],
        flops=4 * full * width * units,
    )
    first_one = swap(first, "group")
    second_one = swap(second, "expert")
    (teach_pre,) = call(
        teacher_in,
        [struct(BF16, 2, slots, units)],
        [own, other, teach_gate, teach_up],
        [pltpu.VMEM((slots, half_width), BF16)],
        flops=4 * slots * half_width * units,
    )
    teach_got = swap(teach_pre, "group")
    first = sum_bf16(first, first_one)
    second = sum_bf16(second, second_one)
    first_two = swap(first, "expert")
    second_two = swap(second, "group")
    teach_keep, teach_send = call(
        teacher_out,
        [struct(F32, slots, block), struct(BF16, slots, block)],
        [teach_pre, teach_got, teach_down],
        flops=2 * slots * half_width * units,
    )
    teach_swap = swap(teach_send, "replica")
    stud_keep, stud_send, hidden = call(
        student_out,
        [struct(F32, full, narrow), struct(BF16, full, narrow), struct(BF16, full, units)],
        [first, first_two, second, second_two, stud_down],
        flops=2 * full * width * units,
    )
    stud_swap = swap(stud_send, "replica")
    (returned,) = call(
        join,
        [struct(BF16, owners, 4 * SLOT, narrow)],
        [stud_keep, stud_swap, teach_keep, teach_swap],
    )
    back = exchange(returned)
    residual, grad_send = call(
        combine,
        [struct(F32, count, block), struct(BF16, owners, 2 * SLOT, narrow)],
        [member_order, back, select, weight],
        [pltpu.VMEM((slots, block), BF16), pltpu.VMEM((slots, block), BF16)],
        smem=1,
        flops=8 * slots * count * block,
    )
    grad_own = exchange(grad_send)
    grad_other = swap(grad_own, "replica")
    back_first, back_second, grad_rows = call(
        hidden_back,
        [struct(BF16, slots, units), struct(BF16, slots, units), struct(BF16, full, width)],
        [grad_own, grad_other, stud_down],
        flops=2 * full * width * units,
    )
    back_first_one = swap(back_first, "group")
    back_second_one = swap(back_second, "expert")
    (grad_down,) = call(
        down_grad,
        [struct(BF16, 1, units, width)],
        [hidden, grad_rows],
        flops=2 * full * width * units,
    )
    back_first = sum_bf16(back_first, back_first_one)
    back_second = sum_bf16(back_second, back_second_one)
    back_first_two = swap(back_first, "expert")
    back_second_two = swap(back_second, "group")
    grad_gate, grad_up = call(
        grads,
        [struct(BF16, 1, units, width), struct(BF16, 1, units, width)],
        [first, first_two, second, second_two, back_first, back_first_two, back_second, back_second_two, stud_rows],
        [pltpu.VMEM((2, full, units), BF16)],
        flops=4 * full * width * units,
    )
    return (residual, grad_gate, grad_up, grad_down)


def solution(mesh):
    weights = P("expert", "replica", "group")
    placed = (P("expert", "group"), P("expert", None), P("expert", None), P()) + (weights,) * 6
    return jax.shard_map(
        shards,
        mesh=mesh,
        in_specs=placed,
        out_specs=(P("expert", ("group", "replica")), weights, weights, weights),
        check_vma=False,
    )
```

```python
import jax
import jax.numpy as jnp
from jax import lax
from jax.experimental import pallas as pl
from jax.experimental.pallas import tpu as pltpu
from jax.sharding import PartitionSpec as P


SLOT = 16


BF16 = jnp.bfloat16
F32 = jnp.float32


def swap(block, axis):
    count = lax.axis_size(axis)
    return lax.ppermute(block, axis, [(place, place ^ 1) for place in range(count)])


def quad(diagonal, group, expert):
    count = 2 * lax.axis_size("expert")
    crossing = [(place, place ^ 3) for place in range(count)]
    diagonal = lax.ppermute(diagonal, ("expert", "group"), crossing)
    return diagonal, swap(group, "group"), swap(expert, "expert")


def exchange(block):
    return lax.all_to_all(block, "expert", split_axis=0, concat_axis=0, tiled=True)


def contract(left, right, dims):
    return lax.dot_general(left, right, ((dims[:1], dims[1:]), ((), ())), preferred_element_type=F32)


def call(body, outs, ins, scratch=(), smem=0, far=0, flops=0, limit=16, space=pltpu.VMEM):
    specs = [pl.BlockSpec(memory_space=pltpu.SMEM)] * smem
    specs += [pl.BlockSpec(memory_space=pltpu.HBM)] * far
    specs += [pl.BlockSpec(memory_space=pltpu.VMEM)] * (len(ins) - smem - far)
    moved = sum(x.size * x.dtype.itemsize for x in ins)
    spaces = [pltpu.HBM] * (smem + far) + [space] * (len(ins) - smem - far)
    placed = map(pltpu.with_memory_space_constraint, ins, spaces)
    return pl.pallas_call(
        body,
        out_shape=outs,
        in_specs=specs,
        out_specs=[pl.BlockSpec(memory_space=pltpu.VMEM)] * len(outs),
        scratch_shapes=scratch,
        cost_estimate=pl.CostEstimate(flops=flops, bytes_accessed=moved, transcendentals=0),
        compiler_params=pltpu.CompilerParams(vmem_limit_bytes=limit << 20),
    )(*placed)


def struct(dtype, *shape):
    return pltpu.VMEM(shape, dtype)


def result(dtype, *shape):
    return jax.ShapeDtypeStruct(shape, dtype)


def spread_members(order, source, target, to_slots):
    owners, _, narrow = target.shape if not to_slots else source.shape
    for dest in range(owners):
        columns = slice(dest % 2 * narrow, (dest % 2 + 1) * narrow)
        for member in range(2):
            start = pl.multiple_of(order[dest // 2 * 2 + member] * SLOT, SLOT)
            rows = slice(member * SLOT, (member + 1) * SLOT)
            if to_slots:
                target[pl.ds(start, SLOT), columns] = source[dest, rows, :]
            else:
                target[dest, rows, :] = source[pl.ds(start, SLOT), columns]


def loads_of(arrived, *pairs):
    loads = [pltpu.make_async_copy(far, near, arrived.at[at]) for at, (far, near) in enumerate(pairs)]
    for load in loads:
        load.start()
    return loads


def expert_hits(ids, slots):
    expert = lax.broadcasted_iota(jnp.int32, (slots, ids.shape[1]), 0) // SLOT
    return [ids[choice : choice + 1, :] == expert for choice in range(ids.shape[0])]


def route(order, gate_hbm, up_hbm, ids, tokens, send, select, gate_near, up_near, picked, arrived):
    loads = loads_of(arrived, (gate_hbm, gate_near), (up_hbm, up_near))
    owners, _, narrow = send.shape
    slots, count = select.shape
    slot = (lax.broadcasted_iota(jnp.int32, (slots, count), 0) % SLOT).astype(F32)
    member = jnp.zeros((slots, count), F32)
    for hit in expert_hits(ids, slots):
        member = jnp.where(hit, 1.0, member)
    before = lax.broadcasted_iota(jnp.int32, (count, count), 0) < lax.broadcasted_iota(
        jnp.int32, (count, count), 1
    )
    rank = contract(member.astype(BF16), before.astype(F32).astype(BF16), (1, 0))
    chosen = (member > 0.0) & (rank == slot)
    onehot = jnp.where(chosen, 1.0, 0.0).astype(BF16)
    select[...] = onehot
    start = pl.multiple_of(lax.axis_index("replica") * 2 * narrow, 2 * narrow)
    picked[...] = contract(onehot, tokens[:, pl.ds(start, 2 * narrow)], (1, 0)).astype(BF16)
    spread_members(order, picked, send, False)
    for dest in range(owners):
        rows = slice(dest * SLOT, (dest + 1) * SLOT)
        send[dest, 2 * SLOT : 3 * SLOT, :] = picked[rows, :narrow]
        send[dest, 3 * SLOT :, :] = picked[rows, narrow:]
    for load in loads:
        load.wait()


def weigh(ids, gates, select, weight):
    gate = jnp.zeros(select.shape, F32)
    for choice, hit in enumerate(expert_hits(ids, select.shape[0])):
        gate = jnp.where(hit, gates[choice : choice + 1, :], gate)
    weight[...] = jnp.sum(jnp.where(select[...].astype(F32) > 0.0, gate, 0.0), axis=1, keepdims=True)


def quad_slices(rows):
    quarter = rows // 4
    mine = lax.axis_index("expert") % 2 * 2 + lax.axis_index("group")
    flip = mine % 2 * 2 - 1
    diagonal = 3 - mine
    expert = diagonal + flip
    group = mine - flip
    return [pl.ds(pl.multiple_of(q * quarter, quarter), quarter) for q in (mine, diagonal, group, expert)]


def student_in(own, other, gate, up, keep, diagonal, group, expert, rows, pre):
    owners, _, narrow = own.shape
    full = 2 * owners * SLOT
    replica = lax.axis_index("replica")
    for part, at in ((own, replica), (other, 1 - replica)):
        columns = pl.ds(pl.multiple_of(at * narrow, narrow), narrow)
        rows[:, columns] = part[:, : 2 * SLOT, :].reshape(full, narrow)
    pieces = quad_slices(full)
    for index, matrix in enumerate((gate, up)):
        pre[...] = contract(rows[...], matrix[0], (1, 1))
        keep[index] = pre[pieces[0], :]
        for piece, out in zip(pieces[1:], (diagonal, group, expert)):
            out[index] = pre[piece, :].astype(BF16)


def student_mid(keep, diagonal, group, expert, pre, hidden):
    gate, up = (
        keep[i] + diagonal[i].astype(F32) + group[i].astype(F32) + expert[i].astype(F32) for i in range(2)
    )
    hidden[...] = hidden_of(gate, up)
    pre[0] = gate.astype(BF16)
    pre[1] = up.astype(BF16)


def half_slices(rows):
    half = rows // 2
    group = lax.axis_index("group")
    return [pl.ds(pl.multiple_of(at * half, half), half) for at in (group, 1 - group)]


def teacher_in(own, other, gate, up, keep, send, rows, pre):
    owners, _, narrow = own.shape
    replica = lax.axis_index("replica")
    for part, at in ((own, replica), (other, 1 - replica)):
        for piece in range(2):
            start = pl.multiple_of((2 * at + piece) * narrow, narrow)
            block = part[:, (2 + piece) * SLOT : (3 + piece) * SLOT, :]
            rows[:, pl.ds(start, narrow)] = block.reshape(owners * SLOT, narrow)
    mine, theirs = half_slices(pre.shape[0])
    for index, matrix in enumerate((gate, up)):
        pre[...] = contract(rows[...], matrix[0], (1, 1))
        keep[index] = pre[mine, :]
        send[index] = pre[theirs, :].astype(BF16)


def teacher_mid(keep, got, hidden):
    gate, up = (keep[i] + got[i].astype(F32) for i in range(2))
    hidden[...] = hidden_of(gate, up)


def hidden_of(gate, up):
    return (gate * jax.nn.sigmoid(gate) * up).astype(BF16)


def divide(hidden, down, keep, send):
    width = keep.shape[1]
    replica = lax.axis_index("replica")
    mine = pl.ds(pl.multiple_of(replica * width, width), width)
    theirs = pl.ds(pl.multiple_of((1 - replica) * width, width), width)
    send[...] = contract(hidden, down[0, :, theirs], (1, 0)).astype(BF16)
    keep[...] = contract(hidden, down[0, :, mine], (1, 0))


def student_out(own, diagonal, group, expert, down, keep, send, hidden):
    pieces = quad_slices(hidden.shape[0])
    for piece, part in zip(pieces, (own, diagonal, group, expert)):
        hidden[piece, :] = part[...]
    divide(hidden[...], down, keep, send)


def teacher_out(own, got, down, keep, send, hidden):
    for piece, part in zip(half_slices(hidden.shape[0]), (own, got)):
        hidden[piece, :] = part[...]
    divide(hidden[...], down, keep, send)


def join(stud, stud_got, teach, teach_got, send):
    owners, _, narrow = send.shape
    total = (stud[...] + stud_got[...].astype(F32)).astype(BF16)
    send[:, : 2 * SLOT, :] = total.reshape(owners, 2 * SLOT, narrow)
    total = (teach[...] + teach_got[...].astype(F32)).astype(BF16)
    for piece in range(2):
        block = total[:, piece * narrow : (piece + 1) * narrow].reshape(owners, SLOT, narrow)
        send[:, (2 + piece) * SLOT : (3 + piece) * SLOT, :] = block


def halves(value):
    high = value.astype(BF16)
    return high, (value - high.astype(F32)).astype(BF16)


def combine(order, back, select, weight, residual, send, stud, teach):
    owners, _, narrow = back.shape
    spread_members(order, back, stud, True)
    for dest in range(owners):
        rows = slice(dest * SLOT, (dest + 1) * SLOT)
        teach[rows, :narrow] = back[dest, 2 * SLOT : 3 * SLOT, :]
        teach[rows, narrow:] = back[dest, 3 * SLOT :, :]
    scale = weight[...]
    high, low = halves(scale * (stud[...].astype(F32) - teach[...].astype(F32)))
    onehot = select[...]
    total = contract(onehot, high, (0, 0)) + contract(onehot, low, (0, 0))
    residual[...] = total
    high, low = halves(total)
    rows = contract(onehot, high, (1, 0)) + contract(onehot, low, (1, 0))
    stud[...] = (scale * rows).astype(BF16)
    spread_members(order, stud, send, False)


def hidden_back(own, other, down, first, second, rows):
    owners, _, narrow = own.shape
    half = owners * SLOT
    replica = lax.axis_index("replica")
    for part, at in ((own, replica), (other, 1 - replica)):
        columns = pl.ds(pl.multiple_of(at * narrow, narrow), narrow)
        rows[:, columns] = part[...].reshape(2 * half, narrow)
    back = contract(rows[...], down[0], (1, 1)).astype(BF16)
    first[...] = back[:half]
    second[...] = back[half:]


def down_grad(hidden, rows, out):
    out[0] = contract(hidden[...], rows[...], (0, 0)).astype(BF16)


def slopes(own, diagonal, group, expert, out):
    pieces = quad_slices(out.shape[1])
    for piece, part in zip(pieces, (own, diagonal, group, expert)):
        gate, up = part[0].astype(F32), part[1].astype(F32)
        sig = jax.nn.sigmoid(gate)
        out[0, piece, :] = up * sig * (1.0 + gate * (1.0 - sig))
        out[1, piece, :] = gate * sig


def grads(slope, a_own, a_got, b_own, b_got, rows, gate_out, up_out, left):
    half = a_own.shape[0]
    for at, (own, got) in enumerate(((a_own, a_got), (b_own, b_got))):
        back = own[...].astype(F32) + got[...].astype(F32)
        block = slice(at * half, (at + 1) * half)
        for index in range(2):
            left[index, block, :] = (back * slope[index, block, :]).astype(BF16)
    gate_out[0] = contract(left[0], rows[...], (0, 0)).astype(BF16)
    up_out[0] = contract(left[1], rows[...], (0, 0)).astype(BF16)


def sum_bf16(own, got):
    return (own.astype(F32) + got.astype(F32)).astype(BF16)


def shards(tokens, expert_ids, route_gates, member_order, teach_gate, teach_up, teach_down, stud_gate, stud_up, stud_down):
    owners = lax.axis_size("expert")
    count, half_width = tokens.shape
    _, units, width = stud_gate.shape
    block = half_width // 2
    narrow = width // 2
    slots = owners * SLOT
    full = 2 * slots
    send, select, gate_near, up_near = call(
        route,
        [
            struct(BF16, owners, 4 * SLOT, narrow),
            struct(BF16, slots, count),
            struct(BF16, 1, units, width),
            struct(BF16, 1, units, width),
        ],
        [member_order, stud_gate, stud_up, expert_ids.T, tokens],
        [pltpu.VMEM((slots, block), BF16), pltpu.SemaphoreType.DMA((2,))],
        smem=1,
        far=2,
        flops=2 * slots * count * block,
        space=pltpu.HBM,
    )
    (weight,) = call(weigh, [struct(F32, slots, 1)], [expert_ids.T, route_gates.T, select])
    own = exchange(send)
    other = swap(own, "replica")
    quarter = full // 4
    pieces = [struct(BF16, 2, quarter, units)] * 3
    keep, *parts, stud_rows = call(
        student_in,
        [struct(F32, 2, quarter, units), *pieces, struct(BF16, full, width)],
        [own, other, gate_near, up_near],
        [pltpu.VMEM((full, units), F32)],
        flops=4 * full * width * units,
    )
    parts = quad(*parts)
    half = slots // 2
    teach_keep, teach_send = call(
        teacher_in,
        [struct(F32, 2, half, units), struct(BF16, 2, half, units)],
        [own, other, teach_gate, teach_up],
        [pltpu.VMEM((slots, half_width), BF16), pltpu.VMEM((slots, units), F32)],
        flops=4 * slots * half_width * units,
    )
    teach_got = swap(teach_send, "group")
    (teach_hidden,) = call(teacher_mid, [struct(BF16, half, units)], [teach_keep, teach_got])
    teach_got = swap(teach_hidden, "group")
    pre, hidden_piece = call(
        student_mid,
        [struct(BF16, 2, quarter, units), struct(BF16, quarter, units)],
        [keep, *parts],
    )
    hidden_parts = (hidden_piece, *quad(*[hidden_piece] * 3))
    pre_parts = (pre, *quad(*[pre] * 3))
    teach_keep, teach_send = call(
        teacher_out,
        [struct(F32, slots, block), struct(BF16, slots, block)],
        [teach_hidden, teach_got, teach_down],
        [pltpu.VMEM((slots, units), BF16)],
        flops=2 * slots * half_width * units,
    )
    teach_swap = swap(teach_send, "replica")
    stud_keep, stud_send, hidden = call(
        student_out,
        [struct(F32, full, narrow), struct(BF16, full, narrow), struct(BF16, full, units)],
        [*hidden_parts, stud_down],
        flops=2 * full * width * units,
    )
    stud_swap = swap(stud_send, "replica")
    (returned,) = call(
        join,
        [struct(BF16, owners, 4 * SLOT, narrow)],
        [stud_keep, stud_swap, teach_keep, teach_swap],
    )
    back = exchange(returned)
    residual, grad_send = call(
        combine,
        [struct(F32, count, block), struct(BF16, owners, 2 * SLOT, narrow)],
        [member_order, back, select, weight],
        [pltpu.VMEM((slots, block), BF16), pltpu.VMEM((slots, block), BF16)],
        smem=1,
        flops=8 * slots * count * block,
    )
    grad_own = exchange(grad_send)
    grad_other = swap(grad_own, "replica")
    back_first, back_second, grad_rows = call(
        hidden_back,
        [struct(BF16, slots, units), struct(BF16, slots, units), struct(BF16, full, width)],
        [grad_own, grad_other, stud_down],
        flops=2 * full * width * units,
    )
    back_first_one = swap(back_first, "group")
    back_second_one = swap(back_second, "expert")
    (grad_down,) = call(
        down_grad,
        [result(BF16, 1, units, width)],
        [hidden, grad_rows],
        flops=2 * full * width * units,
    )
    back_first = sum_bf16(back_first, back_first_one)
    back_second = sum_bf16(back_second, back_second_one)
    back_first_two = swap(back_first, "expert")
    back_second_two = swap(back_second, "group")
    (slope,) = call(slopes, [struct(F32, 2, full, units)], [*pre_parts])
    grad_gate, grad_up = call(
        grads,
        [result(BF16, 1, units, width), result(BF16, 1, units, width)],
        [slope, back_first, back_first_two, back_second, back_second_two, stud_rows],
        [pltpu.VMEM((2, full, units), BF16)],
        flops=4 * full * width * units,
    )
    return (residual, grad_gate, grad_up, grad_down)


def solution(mesh):
    weights = P("expert", "replica", "group")
    placed = (P("expert", "group"), P("expert", None), P("expert", None), P()) + (weights,) * 6
    return jax.shard_map(
        shards,
        mesh=mesh,
        in_specs=placed,
        out_specs=(P("expert", ("group", "replica")), weights, weights, weights),
        check_vma=False,
    )
```

```python
import jax
import jax.numpy as jnp
from jax import lax
from jax.experimental import pallas as pl
from jax.experimental.pallas import tpu as pltpu
from jax.sharding import PartitionSpec as P


SLOT = 16
TILE = 256


BF16 = jnp.bfloat16
F32 = jnp.float32


def swap(block, axis):
    count = lax.axis_size(axis)
    return lax.ppermute(block, axis, [(place, place ^ 1) for place in range(count)])


def quad(diagonal, group, expert):
    count = 2 * lax.axis_size("expert")
    crossing = [(place, place ^ 3) for place in range(count)]
    diagonal = lax.ppermute(diagonal, ("expert", "group"), crossing)
    return diagonal, swap(group, "group"), swap(expert, "expert")


def exchange(block):
    return lax.all_to_all(block, "expert", split_axis=0, concat_axis=0, tiled=True)


def contract(left, right, dims):
    return lax.dot_general(left, right, ((dims[:1], dims[1:]), ((), ())), preferred_element_type=F32)


def call(body, outs, ins, scratch=(), smem=0, far=0, far_outs=0, flops=0, limit=16, space=pltpu.VMEM):
    specs = [pl.BlockSpec(memory_space=pltpu.SMEM)] * smem
    specs += [pl.BlockSpec(memory_space=pltpu.HBM)] * far
    specs += [pl.BlockSpec(memory_space=pltpu.VMEM)] * (len(ins) - smem - far)
    moved = sum(x.size * x.dtype.itemsize for x in ins)
    spaces = [pltpu.HBM] * (smem + far) + [space] * (len(ins) - smem - far)
    placed = map(pltpu.with_memory_space_constraint, ins, spaces)
    return pl.pallas_call(
        body,
        out_shape=outs,
        in_specs=specs,
        out_specs=[pl.BlockSpec(memory_space=pltpu.HBM)] * far_outs
        + [pl.BlockSpec(memory_space=pltpu.VMEM)] * (len(outs) - far_outs),
        scratch_shapes=scratch,
        cost_estimate=pl.CostEstimate(flops=flops, bytes_accessed=moved, transcendentals=0),
        compiler_params=pltpu.CompilerParams(vmem_limit_bytes=limit << 20),
    )(*placed)


def struct(dtype, *shape):
    return pltpu.VMEM(shape, dtype)


def result(dtype, *shape):
    return jax.ShapeDtypeStruct(shape, dtype)


def spread_members(order, source, target, to_slots):
    owners, _, narrow = target.shape if not to_slots else source.shape
    for dest in range(owners):
        columns = slice(dest % 2 * narrow, (dest % 2 + 1) * narrow)
        for member in range(2):
            start = pl.multiple_of(order[dest // 2 * 2 + member] * SLOT, SLOT)
            rows = slice(member * SLOT, (member + 1) * SLOT)
            if to_slots:
                target[pl.ds(start, SLOT), columns] = source[dest, rows, :]
            else:
                target[dest, rows, :] = source[pl.ds(start, SLOT), columns]


def loads_of(arrived, *pairs):
    loads = [pltpu.make_async_copy(far, near, arrived.at[at]) for at, (far, near) in enumerate(pairs)]
    for load in loads:
        load.start()
    return loads


def expert_hits(ids, slots):
    expert = lax.broadcasted_iota(jnp.int32, (slots, ids.shape[1]), 0) // SLOT
    return [ids[choice : choice + 1, :] == expert for choice in range(ids.shape[0])]


def route(order, up_hbm, ids, tokens, send, select, up_near, picked, arrived):
    load = pltpu.make_async_copy(up_hbm, up_near, arrived)
    load.start()
    owners, _, narrow = send.shape
    slots, count = select.shape
    slot = (lax.broadcasted_iota(jnp.int32, (slots, count), 0) % SLOT).astype(F32)
    member = jnp.zeros((slots, count), F32)
    for hit in expert_hits(ids, slots):
        member = jnp.where(hit, 1.0, member)
    before = lax.broadcasted_iota(jnp.int32, (count, count), 0) < lax.broadcasted_iota(
        jnp.int32, (count, count), 1
    )
    rank = contract(member.astype(BF16), before.astype(F32).astype(BF16), (1, 0))
    chosen = (member > 0.0) & (rank == slot)
    onehot = jnp.where(chosen, 1.0, 0.0).astype(BF16)
    select[...] = onehot
    start = pl.multiple_of(lax.axis_index("replica") * 2 * narrow, 2 * narrow)
    picked[...] = contract(onehot, tokens[:, pl.ds(start, 2 * narrow)], (1, 0)).astype(BF16)
    spread_members(order, picked, send, False)
    for dest in range(owners):
        rows = slice(dest * SLOT, (dest + 1) * SLOT)
        send[dest, 2 * SLOT : 3 * SLOT, :] = picked[rows, :narrow]
        send[dest, 3 * SLOT :, :] = picked[rows, narrow:]
    load.wait()


def weigh(ids, gates, select, weight):
    gate = jnp.zeros(select.shape, F32)
    for choice, hit in enumerate(expert_hits(ids, select.shape[0])):
        gate = jnp.where(hit, gates[choice : choice + 1, :], gate)
    weight[...] = jnp.sum(jnp.where(select[...].astype(F32) > 0.0, gate, 0.0), axis=1, keepdims=True)


def quad_slices(rows):
    quarter = rows // 4
    mine = lax.axis_index("expert") % 2 * 2 + lax.axis_index("group")
    flip = mine % 2 * 2 - 1
    diagonal = 3 - mine
    expert = diagonal + flip
    group = mine - flip
    return [pl.ds(pl.multiple_of(q * quarter, quarter), quarter) for q in (mine, diagonal, group, expert)]


def student_in(own, other, gate, up, keep, diagonal, group, expert, rows, pre):
    owners, _, narrow = own.shape
    full = 2 * owners * SLOT
    replica = lax.axis_index("replica")
    for part, at in ((own, replica), (other, 1 - replica)):
        columns = pl.ds(pl.multiple_of(at * narrow, narrow), narrow)
        rows[:, columns] = part[:, : 2 * SLOT, :].reshape(full, narrow)
    pieces = quad_slices(full)
    for index, matrix in enumerate((gate, up)):
        pre[...] = contract(rows[...], matrix[0], (1, 1))
        keep[index] = pre[pieces[0], :]
        for piece, out in zip(pieces[1:], (diagonal, group, expert)):
            out[index] = pre[piece, :].astype(BF16)


def student_mid(keep, diagonal, group, expert, pre, hidden):
    gate, up = (
        keep[i] + diagonal[i].astype(F32) + group[i].astype(F32) + expert[i].astype(F32) for i in range(2)
    )
    hidden[...] = hidden_of(gate, up)
    pre[0] = gate.astype(BF16)
    pre[1] = up.astype(BF16)


def half_slices(rows):
    half = rows // 2
    group = lax.axis_index("group")
    return [pl.ds(pl.multiple_of(at * half, half), half) for at in (group, 1 - group)]


def teacher_in(gate, up, own, other, keep, send, rows, pre, near, arrived):
    loads = loads_of(arrived, (gate.at[0], near.at[0]), (up.at[0], near.at[1]))
    owners, _, narrow = own.shape
    replica = lax.axis_index("replica")
    for part, at in ((own, replica), (other, 1 - replica)):
        for piece in range(2):
            start = pl.multiple_of((2 * at + piece) * narrow, narrow)
            block = part[:, (2 + piece) * SLOT : (3 + piece) * SLOT, :]
            rows[:, pl.ds(start, narrow)] = block.reshape(owners * SLOT, narrow)
    mine, theirs = half_slices(pre.shape[0])
    for index, load in enumerate(loads):
        load.wait()
        pre[...] = contract(rows[...], near[index], (1, 1))
        keep[index] = pre[mine, :]
        send[index] = pre[theirs, :].astype(BF16)


def teacher_mid(keep, got, hidden):
    gate, up = (keep[i] + got[i].astype(F32) for i in range(2))
    hidden[...] = hidden_of(gate, up)


def hidden_of(gate, up):
    return (gate * jax.nn.sigmoid(gate) * up).astype(BF16)


def divide(hidden, down, keep, send):
    width = keep.shape[1]
    replica = lax.axis_index("replica")
    mine = pl.ds(pl.multiple_of(replica * width, width), width)
    theirs = pl.ds(pl.multiple_of((1 - replica) * width, width), width)
    send[...] = contract(hidden, down[0, :, theirs], (1, 0)).astype(BF16)
    keep[...] = contract(hidden, down[0, :, mine], (1, 0))


def student_out(own, diagonal, group, expert, down, keep, send, hidden):
    pieces = quad_slices(hidden.shape[0])
    for piece, part in zip(pieces, (own, diagonal, group, expert)):
        hidden[piece, :] = part[...]
    divide(hidden[...], down, keep, send)


def teacher_out(own, got, down, keep, send, hidden):
    for piece, part in zip(half_slices(hidden.shape[0]), (own, got)):
        hidden[piece, :] = part[...]
    divide(hidden[...], down, keep, send)


def join(stud, stud_got, teach, teach_got, send):
    owners, _, narrow = send.shape
    total = (stud[...] + stud_got[...].astype(F32)).astype(BF16)
    send[:, : 2 * SLOT, :] = total.reshape(owners, 2 * SLOT, narrow)
    total = (teach[...] + teach_got[...].astype(F32)).astype(BF16)
    for piece in range(2):
        block = total[:, piece * narrow : (piece + 1) * narrow].reshape(owners, SLOT, narrow)
        send[:, (2 + piece) * SLOT : (3 + piece) * SLOT, :] = block


def halves(value):
    high = value.astype(BF16)
    return high, (value - high.astype(F32)).astype(BF16)


def combine(order, back, select, weight, residual, send, stud, teach):
    owners, _, narrow = back.shape
    spread_members(order, back, stud, True)
    for dest in range(owners):
        rows = slice(dest * SLOT, (dest + 1) * SLOT)
        teach[rows, :narrow] = back[dest, 2 * SLOT : 3 * SLOT, :]
        teach[rows, narrow:] = back[dest, 3 * SLOT :, :]
    scale = weight[...]
    high, low = halves(scale * (stud[...].astype(F32) - teach[...].astype(F32)))
    onehot = select[...]
    total = contract(onehot, high, (0, 0)) + contract(onehot, low, (0, 0))
    residual[...] = total
    high, low = halves(total)
    rows = contract(onehot, high, (1, 0)) + contract(onehot, low, (1, 0))
    stud[...] = (scale * rows).astype(BF16)
    spread_members(order, stud, send, False)


def hidden_back(own, other, down, first, second, rows):
    owners, _, narrow = own.shape
    half = owners * SLOT
    replica = lax.axis_index("replica")
    for part, at in ((own, replica), (other, 1 - replica)):
        columns = pl.ds(pl.multiple_of(at * narrow, narrow), narrow)
        rows[:, columns] = part[...].reshape(2 * half, narrow)
    back = contract(rows[...], down[0], (1, 1)).astype(BF16)
    first[...] = back[:half]
    second[...] = back[half:]


def down_grad(hidden, rows, out):
    out[0] = contract(hidden[...], rows[...], (0, 0)).astype(BF16)


def stack(own, got, both):
    quarter = own.shape[1]
    both[:, :quarter, :] = own[...]
    both[:, quarter:, :] = got[...]


def slopes(both, got, out):
    quarter = both.shape[1] // 2
    mine, diagonal, group, expert = quad_slices(out.shape[1])
    for part, first, second in ((both, mine, expert), (got, group, diagonal)):
        for at, piece in enumerate((first, second)):
            rows = slice(at * quarter, (at + 1) * quarter)
            gate, up = part[0, rows, :].astype(F32), part[1, rows, :].astype(F32)
            sig = jax.nn.sigmoid(gate)
            out[0, piece, :] = up * sig * (1.0 + gate * (1.0 - sig))
            out[1, piece, :] = gate * sig


def grads(slope, a_own, a_got, b_own, b_got, rows, gate_out, up_out, left, done, leaving):
    half = a_own.shape[0]
    for at, (own, got) in enumerate(((a_own, a_got), (b_own, b_got))):
        back = own[...].astype(F32) + got[...].astype(F32)
        block = slice(at * half, (at + 1) * half)
        for index in range(2):
            left[index, block, :] = (back * slope[index, block, :]).astype(BF16)
    copies = []
    for index, out in enumerate((gate_out, up_out)):
        for start in range(0, left.shape[2], TILE):
            tile = slice(start, start + TILE)
            done[index, tile, :] = contract(left[index, :, tile], rows[...], (0, 0)).astype(BF16)
            semaphore = leaving.at[len(copies)]
            copies.append(pltpu.make_async_copy(done.at[index, tile], out.at[0, tile], semaphore))
            copies[-1].start()
    for copy in copies:
        copy.wait()


def sum_bf16(own, got):
    return (own.astype(F32) + got.astype(F32)).astype(BF16)


def shards(tokens, expert_ids, route_gates, member_order, teach_gate, teach_up, teach_down, stud_gate, stud_up, stud_down):
    owners = lax.axis_size("expert")
    count, half_width = tokens.shape
    _, units, width = stud_gate.shape
    block = half_width // 2
    narrow = width // 2
    slots = owners * SLOT
    full = 2 * slots
    send, select, up_near = call(
        route,
        [
            struct(BF16, owners, 4 * SLOT, narrow),
            struct(BF16, slots, count),
            struct(BF16, 1, units, width),
        ],
        [member_order, stud_up, expert_ids.T, tokens],
        [pltpu.VMEM((slots, block), BF16), pltpu.SemaphoreType.DMA],
        smem=1,
        far=1,
        flops=2 * slots * count * block,
        space=pltpu.HBM,
    )
    (weight,) = call(weigh, [struct(F32, slots, 1)], [expert_ids.T, route_gates.T, select])
    own = exchange(send)
    other = swap(own, "replica")
    quarter = full // 4
    pieces = [struct(BF16, 2, quarter, units)] * 3
    keep, *parts, stud_rows = call(
        student_in,
        [struct(F32, 2, quarter, units), *pieces, struct(BF16, full, width)],
        [own, other, stud_gate, up_near],
        [pltpu.VMEM((full, units), F32)],
        flops=4 * full * width * units,
    )
    parts = quad(*parts)
    half = slots // 2
    teach_keep, teach_send = call(
        teacher_in,
        [struct(F32, 2, half, units), struct(BF16, 2, half, units)],
        [teach_gate, teach_up, own, other],
        [
            pltpu.VMEM((slots, half_width), BF16),
            pltpu.VMEM((slots, units), F32),
            pltpu.VMEM((2, units, half_width), BF16),
            pltpu.SemaphoreType.DMA((2,)),
        ],
        far=2,
        flops=4 * slots * half_width * units,
    )
    teach_got = swap(teach_send, "group")
    (teach_hidden,) = call(teacher_mid, [struct(BF16, half, units)], [teach_keep, teach_got])
    teach_got = swap(teach_hidden, "group")
    pre, hidden_piece = call(
        student_mid,
        [struct(BF16, 2, quarter, units), struct(BF16, quarter, units)],
        [keep, *parts],
    )
    hidden_parts = (hidden_piece, *quad(*[hidden_piece] * 3))
    (pre_both,) = call(stack, [struct(BF16, 2, 2 * quarter, units)], [pre, swap(pre, "expert")])
    pre_got = swap(pre_both, "group")
    teach_keep, teach_send = call(
        teacher_out,
        [struct(F32, slots, block), struct(BF16, slots, block)],
        [teach_hidden, teach_got, teach_down],
        [pltpu.VMEM((slots, units), BF16)],
        flops=2 * slots * half_width * units,
    )
    teach_swap = swap(teach_send, "replica")
    stud_keep, stud_send, hidden = call(
        student_out,
        [struct(F32, full, narrow), struct(BF16, full, narrow), struct(BF16, full, units)],
        [*hidden_parts, stud_down],
        flops=2 * full * width * units,
    )
    stud_swap = swap(stud_send, "replica")
    (returned,) = call(
        join,
        [struct(BF16, owners, 4 * SLOT, narrow)],
        [stud_keep, stud_swap, teach_keep, teach_swap],
    )
    back = exchange(returned)
    residual, grad_send = call(
        combine,
        [struct(F32, count, block), struct(BF16, owners, 2 * SLOT, narrow)],
        [member_order, back, select, weight],
        [pltpu.VMEM((slots, block), BF16), pltpu.VMEM((slots, block), BF16)],
        smem=1,
        flops=8 * slots * count * block,
    )
    grad_own = exchange(grad_send)
    grad_other = swap(grad_own, "replica")
    back_first, back_second, grad_rows = call(
        hidden_back,
        [struct(BF16, slots, units), struct(BF16, slots, units), struct(BF16, full, width)],
        [grad_own, grad_other, stud_down],
        flops=2 * full * width * units,
    )
    back_first_one = swap(back_first, "group")
    back_second_one = swap(back_second, "expert")
    (grad_down,) = call(
        down_grad,
        [result(BF16, 1, units, width)],
        [hidden, grad_rows],
        flops=2 * full * width * units,
    )
    back_first = sum_bf16(back_first, back_first_one)
    back_second = sum_bf16(back_second, back_second_one)
    back_first_two = swap(back_first, "expert")
    back_second_two = swap(back_second, "group")
    (slope,) = call(slopes, [struct(F32, 2, full, units)], [pre_both, pre_got])
    grad_gate, grad_up = call(
        grads,
        [result(BF16, 1, units, width), result(BF16, 1, units, width)],
        [slope, back_first, back_first_two, back_second, back_second_two, stud_rows],
        [
            pltpu.VMEM((2, full, units), BF16),
            pltpu.VMEM((2, units, width), BF16),
            pltpu.SemaphoreType.DMA((2 * -(-units // TILE),)),
        ],
        far_outs=2,
        flops=4 * full * width * units,
    )
    return (residual, grad_gate, grad_up, grad_down)


def solution(mesh):
    weights = P("expert", "replica", "group")
    placed = (P("expert", "group"), P("expert", None), P("expert", None), P()) + (weights,) * 6
    return jax.shard_map(
        shards,
        mesh=mesh,
        in_specs=placed,
        out_specs=(P("expert", ("group", "replica")), weights, weights, weights),
        check_vma=False,
    )
```

```python
import jax
import jax.numpy as jnp
from jax import lax
from jax.experimental import pallas as pl
from jax.experimental.pallas import tpu as pltpu
from jax.sharding import PartitionSpec as P


SLOT = 16
TILE = 256


BF16 = jnp.bfloat16
F32 = jnp.float32


def swap(block, axis):
    count = lax.axis_size(axis)
    return lax.ppermute(block, axis, [(place, place ^ 1) for place in range(count)])


def quad(diagonal, group, expert):
    count = 2 * lax.axis_size("expert")
    crossing = [(place, place ^ 3) for place in range(count)]
    diagonal = lax.ppermute(diagonal, ("expert", "group"), crossing)
    return diagonal, swap(group, "group"), swap(expert, "expert")


def exchange(block):
    return lax.all_to_all(block, "expert", split_axis=0, concat_axis=0, tiled=True)


def contract(left, right, dims):
    return lax.dot_general(left, right, ((dims[:1], dims[1:]), ((), ())), preferred_element_type=F32)


def call(body, outs, ins, scratch=(), smem=0, far=0, far_outs=0, flops=0, limit=16, space=pltpu.VMEM):
    specs = [pl.BlockSpec(memory_space=pltpu.SMEM)] * smem
    specs += [pl.BlockSpec(memory_space=pltpu.HBM)] * far
    specs += [pl.BlockSpec(memory_space=pltpu.VMEM)] * (len(ins) - smem - far)
    moved = sum(x.size * x.dtype.itemsize for x in ins)
    spaces = [pltpu.HBM] * (smem + far) + [space] * (len(ins) - smem - far)
    placed = map(pltpu.with_memory_space_constraint, ins, spaces)
    return pl.pallas_call(
        body,
        out_shape=outs,
        in_specs=specs,
        out_specs=[pl.BlockSpec(memory_space=pltpu.HBM)] * far_outs
        + [pl.BlockSpec(memory_space=pltpu.VMEM)] * (len(outs) - far_outs),
        scratch_shapes=scratch,
        cost_estimate=pl.CostEstimate(flops=flops, bytes_accessed=moved, transcendentals=0),
        compiler_params=pltpu.CompilerParams(vmem_limit_bytes=limit << 20),
    )(*placed)


def struct(dtype, *shape):
    return pltpu.VMEM(shape, dtype)


def result(dtype, *shape):
    return jax.ShapeDtypeStruct(shape, dtype)


def spread_members(order, source, target, to_slots):
    owners, _, narrow = target.shape if not to_slots else source.shape
    for dest in range(owners):
        columns = slice(dest % 2 * narrow, (dest % 2 + 1) * narrow)
        for member in range(2):
            start = pl.multiple_of(order[dest // 2 * 2 + member] * SLOT, SLOT)
            rows = slice(member * SLOT, (member + 1) * SLOT)
            if to_slots:
                target[pl.ds(start, SLOT), columns] = source[dest, rows, :]
            else:
                target[dest, rows, :] = source[pl.ds(start, SLOT), columns]


def loads_of(arrived, *pairs):
    loads = [pltpu.make_async_copy(far, near, arrived.at[at]) for at, (far, near) in enumerate(pairs)]
    for load in loads:
        load.start()
    return loads


def expert_hits(ids, slots):
    expert = lax.broadcasted_iota(jnp.int32, (slots, ids.shape[1]), 0) // SLOT
    return [ids[choice : choice + 1, :] == expert for choice in range(ids.shape[0])]


def route(order, up_hbm, tokens_hbm, ids, send, select, up_near, picked, tokens, arrived):
    owners, _, narrow = send.shape
    start = pl.multiple_of(lax.axis_index("replica") * 2 * narrow, 2 * narrow)
    columns = tokens_hbm.at[:, pl.ds(start, 2 * narrow)]
    loads = loads_of(arrived, (columns, tokens), (up_hbm, up_near))
    slots, count = select.shape
    slot = (lax.broadcasted_iota(jnp.int32, (slots, count), 0) % SLOT).astype(F32)
    member = jnp.zeros((slots, count), F32)
    for hit in expert_hits(ids, slots):
        member = jnp.where(hit, 1.0, member)
    before = lax.broadcasted_iota(jnp.int32, (count, count), 0) < lax.broadcasted_iota(
        jnp.int32, (count, count), 1
    )
    rank = contract(member.astype(BF16), before.astype(F32).astype(BF16), (1, 0))
    chosen = (member > 0.0) & (rank == slot)
    onehot = jnp.where(chosen, 1.0, 0.0).astype(BF16)
    select[...] = onehot
    loads[0].wait()
    picked[...] = contract(onehot, tokens[...], (1, 0)).astype(BF16)
    spread_members(order, picked, send, False)
    for dest in range(owners):
        rows = slice(dest * SLOT, (dest + 1) * SLOT)
        send[dest, 2 * SLOT : 3 * SLOT, :] = picked[rows, :narrow]
        send[dest, 3 * SLOT :, :] = picked[rows, narrow:]
    loads[1].wait()


def weigh(ids, gates, select, weight):
    gate = jnp.zeros(select.shape, F32)
    for choice, hit in enumerate(expert_hits(ids, select.shape[0])):
        gate = jnp.where(hit, gates[choice : choice + 1, :], gate)
    weight[...] = jnp.sum(jnp.where(select[...].astype(F32) > 0.0, gate, 0.0), axis=1, keepdims=True)


def quad_slices(rows):
    quarter = rows // 4
    mine = lax.axis_index("expert") % 2 * 2 + lax.axis_index("group")
    flip = mine % 2 * 2 - 1
    diagonal = 3 - mine
    expert = diagonal + flip
    group = mine - flip
    return [pl.ds(pl.multiple_of(q * quarter, quarter), quarter) for q in (mine, diagonal, group, expert)]


def student_in(own, other, gate, up, keep, diagonal, group, expert, rows, pre):
    owners, _, narrow = own.shape
    full = 2 * owners * SLOT
    replica = lax.axis_index("replica")
    for part, at in ((own, replica), (other, 1 - replica)):
        columns = pl.ds(pl.multiple_of(at * narrow, narrow), narrow)
        rows[:, columns] = part[:, : 2 * SLOT, :].reshape(full, narrow)
    pieces = quad_slices(full)
    for index, matrix in enumerate((gate, up)):
        pre[...] = contract(rows[...], matrix[0], (1, 1))
        keep[index] = pre[pieces[0], :]
        for piece, out in zip(pieces[1:], (diagonal, group, expert)):
            out[index] = pre[piece, :].astype(BF16)


def student_mid(keep, diagonal, group, expert, pre, hidden):
    gate, up = (
        keep[i] + diagonal[i].astype(F32) + group[i].astype(F32) + expert[i].astype(F32) for i in range(2)
    )
    hidden[...] = hidden_of(gate, up)
    pre[0] = gate.astype(BF16)
    pre[1] = up.astype(BF16)


def half_slices(rows):
    half = rows // 2
    group = lax.axis_index("group")
    return [pl.ds(pl.multiple_of(at * half, half), half) for at in (group, 1 - group)]


def teacher_in(gate, up, own, other, keep, send, rows, pre, near, arrived):
    loads = loads_of(arrived, (gate.at[0], near.at[0]), (up.at[0], near.at[1]))
    owners, _, narrow = own.shape
    replica = lax.axis_index("replica")
    for part, at in ((own, replica), (other, 1 - replica)):
        for piece in range(2):
            start = pl.multiple_of((2 * at + piece) * narrow, narrow)
            block = part[:, (2 + piece) * SLOT : (3 + piece) * SLOT, :]
            rows[:, pl.ds(start, narrow)] = block.reshape(owners * SLOT, narrow)
    mine, theirs = half_slices(pre.shape[0])
    for index, load in enumerate(loads):
        load.wait()
        pre[...] = contract(rows[...], near[index], (1, 1))
        keep[index] = pre[mine, :]
        send[index] = pre[theirs, :].astype(BF16)


def teacher_mid(keep, got, hidden):
    gate, up = (keep[i] + got[i].astype(F32) for i in range(2))
    hidden[...] = hidden_of(gate, up)


def hidden_of(gate, up):
    return (gate * jax.nn.sigmoid(gate) * up).astype(BF16)


def divide(hidden, down, keep, send):
    width = keep.shape[1]
    replica = lax.axis_index("replica")
    mine = pl.ds(pl.multiple_of(replica * width, width), width)
    theirs = pl.ds(pl.multiple_of((1 - replica) * width, width), width)
    send[...] = contract(hidden, down[0, :, theirs], (1, 0)).astype(BF16)
    keep[...] = contract(hidden, down[0, :, mine], (1, 0))


def student_out(own, diagonal, group, expert, down, keep, send, hidden):
    pieces = quad_slices(hidden.shape[0])
    for piece, part in zip(pieces, (own, diagonal, group, expert)):
        hidden[piece, :] = part[...]
    divide(hidden[...], down, keep, send)


def teacher_out(own, got, down, keep, send, hidden):
    for piece, part in zip(half_slices(hidden.shape[0]), (own, got)):
        hidden[piece, :] = part[...]
    divide(hidden[...], down, keep, send)


def join(stud, stud_got, teach, teach_got, send):
    owners, _, narrow = send.shape
    total = (stud[...] + stud_got[...].astype(F32)).astype(BF16)
    send[:, : 2 * SLOT, :] = total.reshape(owners, 2 * SLOT, narrow)
    total = (teach[...] + teach_got[...].astype(F32)).astype(BF16)
    for piece in range(2):
        block = total[:, piece * narrow : (piece + 1) * narrow].reshape(owners, SLOT, narrow)
        send[:, (2 + piece) * SLOT : (3 + piece) * SLOT, :] = block


def halves(value):
    high = value.astype(BF16)
    return high, (value - high.astype(F32)).astype(BF16)


def combine(order, back, select, weight, residual, send, stud, teach):
    owners, _, narrow = back.shape
    spread_members(order, back, stud, True)
    for dest in range(owners):
        rows = slice(dest * SLOT, (dest + 1) * SLOT)
        teach[rows, :narrow] = back[dest, 2 * SLOT : 3 * SLOT, :]
        teach[rows, narrow:] = back[dest, 3 * SLOT :, :]
    scale = weight[...]
    high, low = halves(scale * (stud[...].astype(F32) - teach[...].astype(F32)))
    onehot = select[...]
    total = contract(onehot, high, (0, 0)) + contract(onehot, low, (0, 0))
    residual[...] = total
    high, low = halves(total)
    rows = contract(onehot, high, (1, 0)) + contract(onehot, low, (1, 0))
    stud[...] = (scale * rows).astype(BF16)
    spread_members(order, stud, send, False)


def hidden_back(own, other, down, first, second, rows):
    owners, _, narrow = own.shape
    half = owners * SLOT
    replica = lax.axis_index("replica")
    for part, at in ((own, replica), (other, 1 - replica)):
        columns = pl.ds(pl.multiple_of(at * narrow, narrow), narrow)
        rows[:, columns] = part[...].reshape(2 * half, narrow)
    back = contract(rows[...], down[0], (1, 1)).astype(BF16)
    first[...] = back[:half]
    second[...] = back[half:]


def down_grad(hidden, rows, out):
    out[0] = contract(hidden[...], rows[...], (0, 0)).astype(BF16)


def stack(own, got, both):
    quarter = own.shape[1]
    both[:, :quarter, :] = own[...]
    both[:, quarter:, :] = got[...]


def slopes(both, got, out):
    quarter = both.shape[1] // 2
    mine, diagonal, group, expert = quad_slices(out.shape[1])
    for part, first, second in ((both, mine, expert), (got, group, diagonal)):
        for at, piece in enumerate((first, second)):
            rows = slice(at * quarter, (at + 1) * quarter)
            gate, up = part[0, rows, :].astype(F32), part[1, rows, :].astype(F32)
            sig = jax.nn.sigmoid(gate)
            out[0, piece, :] = up * sig * (1.0 + gate * (1.0 - sig))
            out[1, piece, :] = gate * sig


def grads(slope, a_own, a_got, b_own, b_got, rows, gate_out, up_out, left, done, leaving):
    half = a_own.shape[0]
    for at, (own, got) in enumerate(((a_own, a_got), (b_own, b_got))):
        back = own[...].astype(F32) + got[...].astype(F32)
        block = slice(at * half, (at + 1) * half)
        for index in range(2):
            left[index, block, :] = (back * slope[index, block, :]).astype(BF16)
    copies = []
    for index, out in enumerate((gate_out, up_out)):
        for start in range(0, left.shape[2], TILE):
            tile = slice(start, start + TILE)
            done[index, tile, :] = contract(left[index, :, tile], rows[...], (0, 0)).astype(BF16)
            semaphore = leaving.at[len(copies)]
            copies.append(pltpu.make_async_copy(done.at[index, tile], out.at[0, tile], semaphore))
            copies[-1].start()
    for copy in copies:
        copy.wait()


def sum_bf16(own, got):
    return (own.astype(F32) + got.astype(F32)).astype(BF16)


def shards(tokens, expert_ids, route_gates, member_order, teach_gate, teach_up, teach_down, stud_gate, stud_up, stud_down):
    owners = lax.axis_size("expert")
    count, half_width = tokens.shape
    _, units, width = stud_gate.shape
    block = half_width // 2
    narrow = width // 2
    slots = owners * SLOT
    full = 2 * slots
    send, select, up_near = call(
        route,
        [
            struct(BF16, owners, 4 * SLOT, narrow),
            struct(BF16, slots, count),
            struct(BF16, 1, units, width),
        ],
        [member_order, stud_up, tokens, expert_ids.T],
        [pltpu.VMEM((slots, block), BF16), pltpu.VMEM((count, block), BF16), pltpu.SemaphoreType.DMA((2,))],
        smem=1,
        far=2,
        flops=2 * slots * count * block,
        space=pltpu.HBM,
    )
    (weight,) = call(weigh, [struct(F32, slots, 1)], [expert_ids.T, route_gates.T, select])
    own = exchange(send)
    other = swap(own, "replica")
    quarter = full // 4
    pieces = [struct(BF16, 2, quarter, units)] * 3
    keep, *parts, stud_rows = call(
        student_in,
        [struct(F32, 2, quarter, units), *pieces, struct(BF16, full, width)],
        [own, other, stud_gate, up_near],
        [pltpu.VMEM((full, units), F32)],
        flops=4 * full * width * units,
    )
    parts = quad(*parts)
    half = slots // 2
    teach_keep, teach_send = call(
        teacher_in,
        [struct(F32, 2, half, units), struct(BF16, 2, half, units)],
        [teach_gate, teach_up, own, other],
        [
            pltpu.VMEM((slots, half_width), BF16),
            pltpu.VMEM((slots, units), F32),
            pltpu.VMEM((2, units, half_width), BF16),
            pltpu.SemaphoreType.DMA((2,)),
        ],
        far=2,
        flops=4 * slots * half_width * units,
    )
    teach_got = swap(teach_send, "group")
    (teach_hidden,) = call(teacher_mid, [struct(BF16, half, units)], [teach_keep, teach_got])
    teach_got = swap(teach_hidden, "group")
    pre, hidden_piece = call(
        student_mid,
        [struct(BF16, 2, quarter, units), struct(BF16, quarter, units)],
        [keep, *parts],
    )
    hidden_parts = (hidden_piece, *quad(*[hidden_piece] * 3))
    (pre_both,) = call(stack, [struct(BF16, 2, 2 * quarter, units)], [pre, swap(pre, "expert")])
    pre_got = swap(pre_both, "group")
    teach_keep, teach_send = call(
        teacher_out,
        [struct(F32, slots, block), struct(BF16, slots, block)],
        [teach_hidden, teach_got, teach_down],
        [pltpu.VMEM((slots, units), BF16)],
        flops=2 * slots * half_width * units,
    )
    teach_swap = swap(teach_send, "replica")
    stud_keep, stud_send, hidden = call(
        student_out,
        [struct(F32, full, narrow), struct(BF16, full, narrow), struct(BF16, full, units)],
        [*hidden_parts, stud_down],
        flops=2 * full * width * units,
    )
    stud_swap = swap(stud_send, "replica")
    (returned,) = call(
        join,
        [struct(BF16, owners, 4 * SLOT, narrow)],
        [stud_keep, stud_swap, teach_keep, teach_swap],
    )
    back = exchange(returned)
    residual, grad_send = call(
        combine,
        [struct(F32, count, block), struct(BF16, owners, 2 * SLOT, narrow)],
        [member_order, back, select, weight],
        [pltpu.VMEM((slots, block), BF16), pltpu.VMEM((slots, block), BF16)],
        smem=1,
        flops=8 * slots * count * block,
    )
    grad_own = exchange(grad_send)
    grad_other = swap(grad_own, "replica")
    back_first, back_second, grad_rows = call(
        hidden_back,
        [struct(BF16, slots, units), struct(BF16, slots, units), struct(BF16, full, width)],
        [grad_own, grad_other, stud_down],
        flops=2 * full * width * units,
    )
    back_first_one = swap(back_first, "group")
    back_second_one = swap(back_second, "expert")
    (grad_down,) = call(
        down_grad,
        [result(BF16, 1, units, width)],
        [hidden, grad_rows],
        flops=2 * full * width * units,
    )
    back_first = sum_bf16(back_first, back_first_one)
    back_second = sum_bf16(back_second, back_second_one)
    back_first_two = swap(back_first, "expert")
    back_second_two = swap(back_second, "group")
    (slope,) = call(slopes, [struct(F32, 2, full, units)], [pre_both, pre_got])
    grad_gate, grad_up = call(
        grads,
        [result(BF16, 1, units, width), result(BF16, 1, units, width)],
        [slope, back_first, back_first_two, back_second, back_second_two, stud_rows],
        [
            pltpu.VMEM((2, full, units), BF16),
            pltpu.VMEM((2, units, width), BF16),
            pltpu.SemaphoreType.DMA((2 * -(-units // TILE),)),
        ],
        far_outs=2,
        flops=4 * full * width * units,
    )
    return (residual, grad_gate, grad_up, grad_down)


def solution(mesh):
    weights = P("expert", "replica", "group")
    placed = (P("expert", "group"), P("expert", None), P("expert", None), P()) + (weights,) * 6
    return jax.shard_map(
        shards,
        mesh=mesh,
        in_specs=placed,
        out_specs=(P("expert", ("group", "replica")), weights, weights, weights),
        check_vma=False,
    )
```
